512 devices in a mesh: dp: 64 (over z_lo, x, core), ens: 8 (over y, z_hi).
Axes of the slice: x: 4, y: 4, z: 16 (z_hi: 2, z_lo: 8; z = z_hi * 8 + z_lo), core: 2. Of those that a mesh axis runs over, the one named last changes fastest.
Arguments:
- embeddings: bfloat16 [49152, 1024], P('dp'), may hold values from -6 to 6
- valid_mask: int32 [49152], P('dp'), may hold values 0 or 1
- first_weight: bfloat16 [8, 1024, 4096], P(None, 'dp', 'ens'), may hold values from -0.1875 to 0.1875
- second_weight: bfloat16 [8, 4096, 128], P(None, 'ens'), may hold values from -0.09375 to 0.09375
- thresholds: int32 [8], replicated, may hold values from -256 to 256
Outputs:
- mean_logits: float32 [49152, 128], P('dp')
- kept_share: float32 [8], P('ens')
- agree_share: float32 [8], P('ens')
The draws below stay inside these ranges and needn't reach their ends.
All inputs are finite; a program needn't handle non-finite values. No bound on the sum of `valid_mask` on one device may be relied on, other than what follows from the above.
Results may differ from the reference program's by a relative error of at most 0.0044.
Values may be sent and summed in bfloat16 or wider, within the bound.
No kernel may reach another device: no remote copies, remote signals or barrier semaphores. Data moves between devices by JAX's collectives and lax.ppermute only.
A program may use at most 64 MiB of HBM per device.

```python
import jax
import jax.numpy as jnp
from jax import lax

D = 1024
H = 4096
C = 128
DOC_DEV = 768
MEMBERS = 8
DOCS = 49152
N_DP = 64


def with_ends(array, stream_key, low, largest):
    index_at = [jax.random.randint(jax.random.fold_in(stream_key, axis), (), 0, length) for axis, length in enumerate(array.shape)]
    widest = array.shape.index(max(array.shape))
    next_to = index_at[:widest] + [(index_at[widest] + 1) % array.shape[widest]] + index_at[widest + 1:]
    return array.at[tuple(index_at)].set(low).at[tuple(next_to)].set(largest)


def block_scale(own_key, extent, split, least, high):
    loudness = 1.0
    for position, blocks in split:
        heights = jax.random.uniform(jax.random.fold_in(jax.random.fold_in(own_key, 6), position), (blocks,), jnp.float32, least / len(split), high / len(split))
        loudness = loudness * jnp.repeat(jnp.exp(heights), extent[position] // blocks).reshape((-1,) + (1,) * (len(extent) - 1 - position))
    return loudness


def noise(own_key, dims, scale, reach, pieces=(), kind=jnp.bfloat16):
    entries = jax.random.normal(own_key, dims, jnp.float32) * scale
    if len(pieces) > 0:
        entries = block_scale(own_key, dims, pieces, -0.22, 0.18) * entries
    return jnp.clip(entries, min=-reach, max=reach).astype(kind)


def setup_inputs(seed: int = 0) -> dict:
    seeds = jax.random.split(jax.random.key(seed), 6)
    return {
        "embeddings": noise(seeds[0], (DOCS, D), 1.0, 6.0, ((0, 64),)),
        "valid_mask": with_ends((jax.random.randint(seeds[1], (DOCS,), 0, 4) < 3).astype(jnp.int32), jax.random.fold_in(seeds[1], 1), 0, 1),
        "first_weight": noise(seeds[2], (MEMBERS, D, H), D ** -0.5, 0.1875, ((1, 64), (2, 8))),
        "second_weight": noise(seeds[3], (MEMBERS, H, C), H ** -0.5, 0.09375, ((1, 8),)),
        "thresholds": with_ends(jax.random.randint(seeds[4], (MEMBERS,), -256, 257), jax.random.fold_in(seeds[4], 1), -256, 256).astype(jnp.int32),
    }


def member_logits(embeddings, first_weight, second_weight):
    blocks = embeddings.reshape(N_DP, DOC_DEV, D)

    def one_member(weights):
        layer_one, layer_two = weights

        def one_block(block_rows):
            hidden = jnp.maximum(jnp.dot(block_rows, layer_one, preferred_element_type=jnp.float32), 0.0).astype(jnp.bfloat16)
            return jnp.dot(hidden, layer_two, preferred_element_type=jnp.float32)
        return lax.map(one_block, blocks).reshape(DOCS, C)
    return lax.map(one_member, (first_weight, second_weight))

def reference(embeddings, valid_mask, first_weight, second_weight, thresholds):
    logits = member_logits(embeddings, first_weight, second_weight)
    mean_logits = lax.optimization_barrier(jnp.sum(logits, axis=0)) / MEMBERS
    levels = jnp.arange(C, dtype=jnp.float32)
    grades = (2.0 * levels / (C - 1) - 1.0) * jnp.sqrt(jnp.float32(3.0 / C))
    scores = jnp.einsum('edc,c->ed', logits, grades, precision=lax.Precision.HIGHEST)
    ens_score = jnp.dot(mean_logits, grades, precision=lax.Precision.HIGHEST)
    cutoffs = thresholds.astype(jnp.float32) / 256.0
    validity = valid_mask.astype(jnp.float32)
    kept_soft = validity[None, :] * jax.nn.sigmoid(4.0 * (scores - cutoffs[:, None]))
    ens_kept = jax.nn.sigmoid(4.0 * (ens_score - jnp.mean(cutoffs)))
    kept_share = lax.optimization_barrier(jnp.sum(kept_soft, axis=1)) / DOC_DEV
    agree_share = lax.optimization_barrier(jnp.sum(kept_soft * ens_kept[None, :], axis=1)) / DOC_DEV
    return (mean_logits, kept_share, agree_share)
```

```python
import functools

import jax
import jax.numpy as jnp
import ml_dtypes
import numpy as np
from jax import lax
from jax.experimental import pallas as pl
from jax.experimental.pallas import tpu as pltpu
from jax.sharding import Mesh, PartitionSpec as P

F32 = jnp.float32
BF16 = jnp.bfloat16
LANES = 128


def exchange(blocks, axes):
    return lax.all_to_all(blocks, axes, split_axis=0, concat_axis=0, tiled=True)


def to_all(block, axes):
    return exchange(jnp.broadcast_to(block, (lax.axis_size(axes), *block.shape)), axes)


def swap(array, axis):
    return lax.ppermute(array, axis, [(0, 1), (1, 0)])


def grade_parts(classes):
    levels = np.arange(classes, dtype=np.float32)
    rest = (np.float32(2.0) * levels / np.float32(classes - 1) - np.float32(1.0)) * np.sqrt(np.float32(3.0 / classes))
    parts = np.zeros((classes, LANES), np.float32)
    for k in range(3):
        part = rest.astype(ml_dtypes.bfloat16).astype(np.float32)
        parts[:, k] = part
        rest = rest - part
    return parts.astype(ml_dtypes.bfloat16)


def score_kernel(core_ref, docs_ref, own_ref, other_ref, second_ref, grades_ref, mean_ref, scores_ref, first, total, marks):
    member = pl.program_id(0)
    n_x, n_z = own_ref.shape[0], own_ref.shape[1]
    core = core_ref[0]
    for x in range(n_x):
        for z in range(n_z):
            first[z, x, core] = own_ref[x, z, 0]
            first[z, x, 1 - core] = other_ref[x, z, 0]
    width = first.shape[-1]
    weight = first[...].reshape(docs_ref.shape[1], width)
    hidden = jnp.maximum(jnp.dot(docs_ref[...], weight, preferred_element_type=F32), 0.0).astype(BF16)
    second = second_ref[0]
    direction = jnp.sum(jnp.dot(second, grades_ref[...], preferred_element_type=F32), axis=1, keepdims=True)
    high = direction.astype(BF16)
    low = (direction - high.astype(F32)).astype(BF16)
    lane = lax.broadcasted_iota(jnp.int32, (width, LANES), 1)
    zero = jnp.zeros((width, LANES), F32)
    along = jnp.where(lane == 2 * member, high.astype(F32), jnp.where(lane == 2 * member + 1, low.astype(F32), zero)).astype(BF16)
    both = jnp.concatenate([second, along], axis=1)
    part = jnp.dot(hidden, both, preferred_element_type=F32)

    @pl.when(member == 0)
    def _():
        total[...] = part

    @pl.when(member > 0)
    def _():
        total[...] += part

    @pl.when(member == pl.num_programs(0) - 1)
    def _():
        mean_ref[...] = total[:, :LANES].astype(BF16)
        scores_ref[...] = lax.dot_general(
            marks[...], total[:, LANES:], (((1,), (1,)), ((), ())),
            precision=lax.Precision.HIGHEST, preferred_element_type=F32,
        )

    @pl.when(member == 0)
    def _():
        row = lax.broadcasted_iota(jnp.int32, marks.shape, 0)
        col = lax.broadcasted_iota(jnp.int32, marks.shape, 1)
        marks[...] = jnp.where(col // 2 == row, 1.0, 0.0).astype(F32)


def score(core, docs, own, other, second, grades):
    n_x, n_z, members, rows, width = own.shape
    n_docs, depth = docs.shape
    block = (n_x, n_z, 1, rows, width)
    whole = lambda m, c: (0, 0)
    piece = lambda m, c: (0, 0, m, 0, 0)
    return pl.pallas_call(
        score_kernel,
        grid_spec=pltpu.PrefetchScalarGridSpec(
            num_scalar_prefetch=1,
            grid=(members,),
            in_specs=[
                pl.BlockSpec((n_docs, depth), whole),
                pl.BlockSpec(block, piece),
                pl.BlockSpec(block, piece),
                pl.BlockSpec((1, width, LANES), lambda m, c: (m, 0, 0)),
                pl.BlockSpec((LANES, LANES), whole),
            ],
            out_specs=[pl.BlockSpec((n_docs, LANES), whole), pl.BlockSpec((8, n_docs), whole)],
            scratch_shapes=[
                pltpu.VMEM((n_z, n_x, 2, rows, width), BF16),
                pltpu.VMEM((n_docs, 2 * LANES), F32),
                pltpu.VMEM((8, LANES), F32),
            ],
        ),
        out_shape=[jax.ShapeDtypeStruct((n_docs, LANES), BF16), jax.ShapeDtypeStruct((8, n_docs), F32)],
        compiler_params=pltpu.CompilerParams(dimension_semantics=("arbitrary",), vmem_limit_bytes=40 * 1024 * 1024),
    )(core, docs, own, other, second, grades)


def halves(scores):
    high = lax.reduce_precision(scores, 8, 7)
    low = lax.reduce_precision(scores - high, 8, 7)
    return jnp.stack([high, low]).astype(BF16)


def on_device(embeddings, valid_mask, first_weight, second_weight, thresholds):
    members, rows, width = first_weight.shape
    n_docs = embeddings.shape[0]
    half = members // 2
    z_axes = ("za", "zp")
    n_za, n_x, n_y = lax.axis_size("za"), lax.axis_size("x"), lax.axis_size("y")
    parity = lax.axis_index("zp")
    core = lax.axis_index("core").reshape(1).astype(jnp.int32)

    blocks = first_weight.reshape(1, 2, half, rows, width)
    blocks = jnp.broadcast_to(blocks, (n_za, *blocks.shape[1:])).reshape(n_za * 2, half, rows, width)
    along_z = exchange(blocks, z_axes)
    docs, along_z = lax.optimization_barrier((embeddings, along_z))
    docs_near = swap(docs, "zp")
    own = to_all(along_z, "x")
    other = swap(own, "core")
    second = lax.dynamic_slice_in_dim(second_weight, parity * half, half, 0)
    grades = jnp.asarray(grade_parts(second_weight.shape[2]))
    mean_own, scores_own = score(core, docs, own, other, second, grades)
    mean_near, scores_near = score(core, docs_near, own, other, second, grades)

    quarter = n_docs // n_y
    score_rows = half * n_docs // LANES

    def packed(mean, scores):
        parts = halves(scores[:half]).reshape(1, 2 * score_rows, LANES)
        parts = jnp.broadcast_to(parts, (n_y, *parts.shape[1:]))
        return jnp.concatenate([mean.reshape(n_y, quarter, LANES), parts], axis=1)

    mine, near = packed(mean_own, scores_own), packed(mean_near, scores_near)
    even = parity == 0
    blocks = jnp.concatenate([jnp.where(even, mine, near), jnp.where(even, near, mine)], axis=0)
    blocks = exchange(blocks, ("zp", "y"))
    part_mean = lax.reduce_precision(jnp.sum(blocks[:, :quarter].astype(F32), axis=0), 8, 7).astype(BF16)
    part_scores = blocks[:, quarter:].astype(F32).reshape(2, n_y * 2, score_rows, LANES).sum(axis=1)
    packed_scores = halves(part_scores.reshape(2 * score_rows, LANES)).reshape(4 * score_rows, LANES)
    message = jnp.concatenate([part_mean, packed_scores], axis=0)
    answer = swap(message, "zh")
    both = message.astype(F32) + answer.astype(F32)
    mean_quarter = (both[:quarter] * (1.0 / members)).astype(BF16)
    mean_logits = to_all(mean_quarter, "y").reshape(n_docs, LANES).astype(F32)
    scores = (both[quarter : quarter + 2 * score_rows] + both[quarter + 2 * score_rows :]).reshape(members, n_docs)

    cutoffs = thresholds.astype(F32) / 256.0
    validity = valid_mask.astype(F32)
    kept_soft = validity[None, :] * jax.nn.sigmoid(4.0 * (scores - cutoffs[:, None]))
    ens_score = jnp.sum(scores, axis=0) / members
    ens_kept = jax.nn.sigmoid(4.0 * (ens_score - jnp.mean(cutoffs)))
    counts = jnp.stack([jnp.sum(kept_soft, axis=1), jnp.sum(kept_soft * ens_kept[None, :], axis=1)])
    counts = to_all(counts, ("x", "core")).sum(axis=0)
    counts = to_all(counts, z_axes).sum(axis=0)
    member = lax.axis_index("y") * 2 + lax.axis_index("zh")
    shares = lax.dynamic_slice_in_dim(counts, member, 1, 1) / n_docs
    return mean_logits, shares[0], shares[1]


def solution(mesh):
    devices = mesh.devices.reshape(4, 2, 4, 2, 4, 2)
    fine = Mesh(devices, ("za", "zp", "x", "core", "y", "zh"))
    dp, ens = ("za", "zp", "x", "core"), ("y", "zh")
    return jax.shard_map(
        on_device,
        mesh=fine,
        in_specs=(P(dp, None), P(dp), P(None, dp, ens), P(None, ens, None), P()),
        out_specs=(P(dp, None), P(ens), P(ens)),
        check_vma=False,
    )
```

```python
import jax
import jax.numpy as jnp
import ml_dtypes
import numpy as np
from jax import lax
from jax.experimental import pallas as pl
from jax.experimental.pallas import tpu as pltpu
from jax.sharding import Mesh, PartitionSpec as P


F32 = jnp.float32
BF16 = jnp.bfloat16
LANES = 128


def exchange(blocks, axes):
    return lax.all_to_all(blocks, axes, split_axis=0, concat_axis=0, tiled=True)


def to_all(block, axes):
    return exchange(jnp.broadcast_to(block, (lax.axis_size(axes), *block.shape)), axes)


def swap(array, axis):
    return lax.ppermute(array, axis, [(0, 1), (1, 0)])


def grade_parts(classes):
    levels = np.arange(classes, dtype=np.float32)
    rest = (np.float32(2.0) * levels / np.float32(classes - 1) - np.float32(1.0)) * np.sqrt(np.float32(3.0 / classes))
    parts = np.zeros((classes, LANES), np.float32)
    for k in range(3):
        part = rest.astype(ml_dtypes.bfloat16).astype(np.float32)
        parts[:, k] = part
        rest = rest - part
    return parts.astype(ml_dtypes.bfloat16)


def score_kernel(base_ref, own_docs_ref, near_docs_ref, first_ref, second_ref, grades_ref, mean_ref, scores_ref, first, both, total, marks):
    member = pl.program_id(0)
    n_x, n_zc = first_ref.shape[0], first_ref.shape[1]
    _, depth = own_docs_ref.shape
    width = first.shape[-1]
    for x in range(n_x):
        for z in range(n_zc // 2):
            for core in range(2):
                first[z, x, core] = first_ref[x, 2 * z + core, 0]
    second = second_ref[0]
    direction = jnp.sum(jnp.dot(second, grades_ref[...], preferred_element_type=F32), axis=1, keepdims=True)
    high = direction.astype(BF16).astype(F32)
    low = direction - high
    lane = lax.broadcasted_iota(jnp.int32, (width, LANES), 1)
    along = jnp.where(lane == 2 * member, high, jnp.where(lane == 2 * member + 1, low, 0.0))
    both[:, :LANES] = second
    both[:, LANES:] = along.astype(BF16)

    @pl.when(member == 0)
    def _():
        total[...] = jnp.zeros_like(total)
        row = lax.broadcasted_iota(jnp.int32, marks.shape, 0)
        col = lax.broadcasted_iota(jnp.int32, marks.shape, 1)
        marks[...] = jnp.where(col // 2 == row, 1.0, 0.0).astype(F32)

    for k, docs_ref in enumerate((own_docs_ref, near_docs_ref)):
        weight = first[...].reshape(depth, width)
        hidden = jnp.maximum(jnp.dot(docs_ref[...], weight, preferred_element_type=F32), 0.0).astype(BF16)
        total[k] += jnp.dot(hidden, both[...], preferred_element_type=F32)

    @pl.when(member == pl.num_programs(0) - 1)
    def _():
        for k in range(2):
            mean_ref[k] = total[k, :, :LANES]
            scores_ref[k] = lax.dot_general(
                marks[...], total[k, :, LANES:], (((1,), (1,)), ((), ())),
                precision=lax.Precision.HIGHEST, preferred_element_type=F32,
            )


def score(base, own_docs, near_docs, first, second, grades):
    n_x, n_zc, members, rows, width = first.shape
    n_docs, depth = own_docs.shape
    whole = lambda m, b: (0, 0)
    return pl.pallas_call(
        score_kernel,
        grid_spec=pltpu.PrefetchScalarGridSpec(
            num_scalar_prefetch=1,
            grid=(members,),
            in_specs=[
                pl.BlockSpec((n_docs, depth), whole),
                pl.BlockSpec((n_docs, depth), whole),
                pl.BlockSpec((n_x, n_zc, 1, rows, width), lambda m, b: (0, 0, m, 0, 0)),
                pl.BlockSpec((1, width, LANES), lambda m, b: (b[0] + m, 0, 0)),
                pl.BlockSpec((LANES, LANES), whole),
            ],
            out_specs=[
                pl.BlockSpec((2, n_docs, LANES), lambda m, b: (0, 0, 0)),
                pl.BlockSpec((2, 8, n_docs), lambda m, b: (0, 0, 0)),
            ],
            scratch_shapes=[
                pltpu.VMEM((n_zc // 2, n_x, 2, rows, width), BF16),
                pltpu.VMEM((width, 2 * LANES), BF16),
                pltpu.VMEM((2, n_docs, 2 * LANES), F32),
                pltpu.VMEM((8, LANES), F32),
            ],
        ),
        out_shape=[jax.ShapeDtypeStruct((2, n_docs, LANES), F32), jax.ShapeDtypeStruct((2, 8, n_docs), F32)],
        compiler_params=pltpu.CompilerParams(dimension_semantics=("arbitrary",), vmem_limit_bytes=40 * 1024 * 1024),
    )(base, own_docs, near_docs, first, second, grades)


def halves(scores):
    high = lax.reduce_precision(scores, 8, 7)
    low = lax.reduce_precision(scores - high, 8, 7)
    return jnp.stack([high, low]).astype(BF16)


def step(embeddings, valid_mask, first_weight, second_weight, thresholds):
    members, rows, width = first_weight.shape
    n_docs = embeddings.shape[0]
    z_axes = ("za", "zp")
    n_za, n_y = lax.axis_size("za"), lax.axis_size("y")
    parity, core = lax.axis_index("zp"), lax.axis_index("core")
    half, pair = members // 2, members // 4

    blocks = first_weight.reshape(1, 4, pair, rows, width)
    blocks = jnp.broadcast_to(blocks, (n_za, *blocks.shape[1:])).reshape(n_za * 4, pair, rows, width)
    along_z = exchange(blocks, ("za", "zp", "core"))
    docs, along_z = lax.optimization_barrier((embeddings, along_z))
    docs_near = swap(docs, "zp")
    first_a = to_all(along_z, "x")
    first_b = swap(first_a, "core")
    grades = jnp.asarray(grade_parts(second_weight.shape[2]))

    def scored(first, which):
        base = (parity * half + which * pair).reshape(1).astype(jnp.int32)
        return score(base, docs, docs_near, first, second_weight, grades)

    mean_a, scores_a = scored(first_a, core)
    mean_b, scores_b = scored(first_b, 1 - core)

    quarter = n_docs // n_y
    score_rows = half * n_docs // LANES
    scores_a, scores_b = scores_a[:, :pair], scores_b[:, :pair]
    low_core = core == 0
    scores = jnp.concatenate([jnp.where(low_core, scores_a, scores_b), jnp.where(low_core, scores_b, scores_a)], axis=1)
    parts = jnp.moveaxis(halves(scores), 0, 1).reshape(2, 1, 2 * score_rows, LANES)
    parts = jnp.broadcast_to(parts, (2, n_y, 2 * score_rows, LANES))
    packed = jnp.concatenate([(mean_a + mean_b).astype(BF16).reshape(2, n_y, quarter, LANES), parts], axis=2)
    even = parity == 0
    blocks = jnp.concatenate([jnp.where(even, packed[0], packed[1]), jnp.where(even, packed[1], packed[0])], axis=0)
    blocks = exchange(blocks, ("zp", "y"))
    part_mean = lax.reduce_precision(jnp.sum(blocks[:, :quarter].astype(F32), axis=0), 8, 7).astype(BF16)
    part_scores = blocks[:, quarter:].astype(F32).reshape(2, n_y * 2, score_rows, LANES).sum(axis=1)
    packed_scores = halves(part_scores.reshape(2 * score_rows, LANES)).reshape(4 * score_rows, LANES)
    message = jnp.concatenate([part_mean, packed_scores], axis=0)
    answer = swap(message, "zh")
    total = message.astype(F32) + answer.astype(F32)
    mean_quarter = (total[:quarter] * (1.0 / members)).astype(BF16)
    turn = [mean_quarter]
    for k in range(1, n_y):
        turn.append(lax.ppermute(mean_quarter, "y", [(i, (i + k) % n_y) for i in range(n_y)]))
    back = [(lax.axis_index("y") + n_y - q) % n_y for q in range(n_y)]
    mean_logits = jnp.concatenate([lax.select_n(k, *turn).astype(F32) for k in back], axis=0)
    scores = (total[quarter : quarter + 2 * score_rows] + total[quarter + 2 * score_rows :]).reshape(members, n_docs)

    cutoffs = thresholds.astype(F32) / 256.0
    validity = valid_mask.astype(F32)
    kept_soft = validity[None, :] * jax.nn.sigmoid(4.0 * (scores - cutoffs[:, None]))
    ens_score = jnp.sum(scores, axis=0) / members
    ens_kept = jax.nn.sigmoid(4.0 * (ens_score - jnp.mean(cutoffs)))
    counts = jnp.stack([jnp.sum(kept_soft, axis=1), jnp.sum(kept_soft * ens_kept[None, :], axis=1)])
    counts = to_all(counts, ("x", "core")).sum(axis=0)
    counts = to_all(counts, z_axes).sum(axis=0)
    member = lax.axis_index("y") * 2 + lax.axis_index("zh")
    shares = lax.dynamic_slice_in_dim(counts, member, 1, 1) / n_docs
    return mean_logits, shares[0], shares[1]


def solution(mesh):
    devices = mesh.devices.reshape(4, 2, 4, 2, 4, 2)
    fine = Mesh(devices, ("za", "zp", "x", "core", "y", "zh"))
    dp, ens = ("za", "zp", "x", "core"), ("y", "zh")
    return jax.shard_map(
        step,
        mesh=fine,
        in_specs=(P(dp, None), P(dp), P(None, dp, ens), P(None, ens, None), P()),
        out_specs=(P(dp, None), P(ens), P(ens)),
        check_vma=False,
    )
```

```python
import functools

import jax
import jax.numpy as jnp
import ml_dtypes
import numpy as np
from jax import lax
from jax.experimental import pallas as pl
from jax.experimental.pallas import tpu as pltpu
from jax.sharding import Mesh, PartitionSpec as P


F32 = jnp.float32
BF16 = jnp.bfloat16


def exchange(blocks, axes):
    return lax.all_to_all(blocks, axes, split_axis=0, concat_axis=0, tiled=True)


def to_all(block, axes):
    return exchange(jnp.broadcast_to(block, (lax.axis_size(axes), *block.shape)), axes)


def swap(array, axis):
    return lax.ppermute(array, axis, [(0, 1), (1, 0)])


def grade_rows(classes):
    levels = np.arange(classes, dtype=np.float32)
    rest = (np.float32(2.0) * levels / np.float32(classes - 1) - np.float32(1.0)) * np.sqrt(np.float32(3.0 / classes))
    rows = np.zeros((classes + 8, classes), np.float32)
    rows[:classes] = np.eye(classes)
    for k in range(3):
        rows[classes + k] = rest.astype(ml_dtypes.bfloat16).astype(np.float32)
        rest = rest - rows[classes + k]
    return rows.astype(ml_dtypes.bfloat16)


CROSS = (((1,), (1,)), ((), ()))


def score_kernel(last, scalars, own_docs_ref, near_docs_hbm, first_ref, second_ref, grades_ref, *refs):
    if last:
        before_ref, packed_ref, total, first, both, near_docs, arrived = refs
        own_docs = own_docs_ref
    else:
        total, first, both, near_docs, arrived, own_docs, own_arrived = refs
        fetch_own = pltpu.make_async_copy(own_docs_ref, own_docs, own_arrived)
    member = pl.program_id(0)
    which, parity = scalars[1], scalars[2]
    n_x, n_zc = first_ref.shape[0], first_ref.shape[1]
    _, depth = near_docs.shape
    width = first.shape[-1]
    classes = second_ref.shape[-1]
    fetch_near = pltpu.make_async_copy(near_docs_hbm, near_docs, arrived)

    @pl.when(member == 0)
    def _():
        if not last:
            fetch_own.start()
        fetch_near.start()

    at = 0 if last else member
    for x in range(n_x):
        for z in range(n_zc // 2):
            for core in range(2):
                first[z, x, core] = first_ref[x, 2 * z + core, at]
    rows = lax.dot_general(grades_ref[...], second_ref[0], CROSS, preferred_element_type=F32)
    direction = rows[classes : classes + 1] + rows[classes + 1 : classes + 2] + rows[classes + 2 : classes + 3]
    high = direction.astype(BF16).astype(F32)
    low = direction - high
    row = lax.broadcasted_iota(jnp.int32, (8, width), 0)
    slot = 2 * which + member
    along = jnp.where(row == slot, high, jnp.where(row == slot + 4, low, 0.0))
    both[...] = jnp.concatenate([rows[:classes], along], axis=0).astype(BF16)

    def add(k, docs):
        weight = first[...].reshape(depth, width)
        hidden = jnp.maximum(jnp.dot(docs, weight, preferred_element_type=F32), 0.0).astype(BF16)
        part = lax.dot_general(both[...], hidden, CROSS, preferred_element_type=F32)

        @pl.when(member == 0)
        def _():
            total[k] = part + before_ref[k] if last else part

        @pl.when(member > 0)
        def _():
            total[k] += part

    if not last:

        @pl.when(member == 0)
        def _():
            fetch_own.wait()

    add(0, own_docs[...])

    @pl.when(member == 0)
    def _():
        fetch_near.wait()

    add(1, near_docs[...])
    if not last:
        return

    @pl.when(member == pl.num_programs(0) - 1)
    def _():
        n_y = packed_ref.shape[0] // 2
        quarter = classes // n_y
        for k in range(2):
            owner = (parity if k == 0 else 1 - parity) * n_y
            scores = total[k, classes : classes + 4] + total[k, classes + 4 : classes + 8]
            top = scores.astype(BF16).astype(F32)
            parts = jnp.concatenate([top, scores - top], axis=0).astype(BF16)
            for q in range(n_y):
                packed_ref[owner + q, :quarter] = total[k, quarter * q : quarter * (q + 1)].astype(BF16)
                packed_ref[owner + q, quarter:] = parts


def score(last, scalars, own_docs, near_docs, first, second, grades, n_y, *before):
    n_x, n_zc, members, rows, width = first.shape
    n_docs, depth = own_docs.shape
    classes = second.shape[-1]
    vmem = pl.BlockSpec(memory_space=pltpu.VMEM)
    hbm = pl.BlockSpec(memory_space=pltpu.HBM)
    totals = (2, classes + 8, n_docs)
    packed = (2 * n_y, classes // n_y + 8, n_docs)
    first_spec = pl.BlockSpec((n_x, n_zc, 1, rows, width), lambda m, s: (0, 0, m, 0, 0)) if last else vmem
    docs_scratch = [pltpu.VMEM((n_docs, depth), BF16), pltpu.SemaphoreType.DMA]
    scratch = [pltpu.VMEM((n_zc // 2, n_x, 2, rows, width), BF16), pltpu.VMEM((classes + 8, width), BF16)] + docs_scratch
    return pl.pallas_call(
        functools.partial(score_kernel, last),
        grid_spec=pltpu.PrefetchScalarGridSpec(
            num_scalar_prefetch=1,
            grid=(members,),
            in_specs=[
                vmem if last else hbm,
                hbm,
                first_spec,
                pl.BlockSpec((1, width, classes), lambda m, s: (s[0] + m, 0, 0)),
                vmem,
            ]
            + [vmem] * len(before),
            out_specs=vmem,
            scratch_shapes=[pltpu.VMEM(totals, F32)] + scratch if last else scratch + docs_scratch,
        ),
        out_shape=jax.ShapeDtypeStruct(packed, BF16) if last else jax.ShapeDtypeStruct(totals, F32),
        compiler_params=pltpu.CompilerParams(dimension_semantics=("arbitrary",), vmem_limit_bytes=32 * 1024 * 1024),
    )(scalars, own_docs, near_docs, first, second, grades, *before)


def order_kernel(mine, *refs):
    *turn, out_ref = refs
    n_y = len(turn)
    quarters = []
    for q in range(n_y):
        back = lax.rem(mine[0] + n_y - q, n_y)
        quarter = turn[0][...].astype(F32)
        for k in range(1, n_y):
            quarter = jnp.where(back == k, turn[k][...].astype(F32), quarter)
        quarters.append(quarter)
    out_ref[...] = jnp.concatenate(quarters, axis=0).T


def in_order(mine, turn):
    rows, n_docs = turn[0].shape
    vmem = pl.BlockSpec(memory_space=pltpu.VMEM)
    return pl.pallas_call(
        order_kernel,
        in_specs=[pl.BlockSpec(memory_space=pltpu.SMEM)] + [vmem] * len(turn),
        out_specs=vmem,
        out_shape=jax.ShapeDtypeStruct((n_docs, rows * len(turn)), F32),
        compiler_params=pltpu.CompilerParams(vmem_limit_bytes=8 * 1024 * 1024),
    )(mine.reshape(1).astype(jnp.int32), *turn)


def halves(scores):
    high = lax.reduce_precision(scores, 8, 7)
    low = lax.reduce_precision(scores - high, 8, 7)
    return jnp.stack([high, low]).astype(BF16)


def step(embeddings, valid_mask, first_weight, second_weight, thresholds):
    members, rows, width = first_weight.shape
    n_docs = embeddings.shape[0]
    z_axes = ("za", "zp")
    n_za, n_y = lax.axis_size("za"), lax.axis_size("y")
    parity, core = lax.axis_index("zp"), lax.axis_index("core")
    half, pair = members // 2, members // 4

    blocks = first_weight.reshape(1, 4, pair, rows, width)
    blocks = jnp.broadcast_to(blocks, (n_za, *blocks.shape[1:])).reshape(n_za * 4, pair, rows, width)
    along_z = exchange(blocks, ("za", "zp", "core"))
    docs, along_z = lax.optimization_barrier((embeddings, along_z))
    docs_near = swap(docs, "zp")
    first_a = to_all(along_z, "x")
    first_b = swap(first_a, "core")
    classes = second_weight.shape[2]
    grades = jnp.asarray(grade_rows(classes))

    def scored(last, first, which, *before):
        scalars = jnp.stack([parity * half + which * pair, which, parity]).astype(jnp.int32)
        return score(last, scalars, docs, docs_near, first, second_weight, grades, n_y, *before)

    total_a = scored(False, first_a, core)
    packed = scored(True, first_b, 1 - core, total_a)

    quarter = classes // n_y
    blocks = exchange(packed, ("zp", "y"))
    part_mean = lax.reduce_precision(jnp.sum(blocks[:, :quarter].astype(F32), axis=0), 8, 7).astype(BF16)
    part_scores = blocks[:, quarter:].astype(F32).reshape(2, n_y, 2, half, n_docs).sum(axis=(1, 2)).reshape(members, n_docs)
    message = jnp.concatenate([part_mean, halves(part_scores).reshape(2 * members, n_docs)], axis=0)
    answer = swap(message, "zh")
    total = message.astype(F32) + answer.astype(F32)
    mean_quarter = (total[:quarter] * (1.0 / members)).astype(BF16)
    turn = [mean_quarter]
    for k in range(1, n_y):
        turn.append(lax.ppermute(mean_quarter, "y", [(i, (i + k) % n_y) for i in range(n_y)]))
    mean_logits = in_order(lax.axis_index("y"), turn)
    scores = total[quarter : quarter + members] + total[quarter + members :]

    cutoffs = thresholds.astype(F32) / 256.0
    validity = valid_mask.astype(F32)
    kept_soft = validity[None, :] * jax.nn.sigmoid(4.0 * (scores - cutoffs[:, None]))
    ens_score = jnp.sum(scores, axis=0) / members
    ens_kept = jax.nn.sigmoid(4.0 * (ens_score - jnp.mean(cutoffs)))
    counts = jnp.stack([jnp.sum(kept_soft, axis=1), jnp.sum(kept_soft * ens_kept[None, :], axis=1)])
    counts = to_all(counts, ("x", "core")).sum(axis=0)
    counts = to_all(counts, z_axes).sum(axis=0)
    member = lax.axis_index("y") * 2 + lax.axis_index("zh")
    shares = lax.dynamic_slice_in_dim(counts, member, 1, 1) / n_docs
    return mean_logits, shares[0], shares[1]


def solution(mesh):
    devices = mesh.devices.reshape(4, 2, 4, 2, 4, 2)
    fine = Mesh(devices, ("za", "zp", "x", "core", "y", "zh"))
    dp, ens = ("za", "zp", "x", "core"), ("y", "zh")
    return jax.shard_map(
        step,
        mesh=fine,
        in_specs=(P(dp, None), P(dp), P(None, dp, ens), P(None, ens, None), P()),
        out_specs=(P(dp, None), P(ens), P(ens)),
        check_vma=False,
    )
```

```python
import functools

import jax
import jax.numpy as jnp
import ml_dtypes
import numpy as np
from jax import lax
from jax.experimental import pallas as pl
from jax.experimental.pallas import tpu as pltpu
from jax.sharding import Mesh, PartitionSpec as P


F32 = jnp.float32
BF16 = jnp.bfloat16


def exchange(blocks, axes):
    return lax.all_to_all(blocks, axes, split_axis=0, concat_axis=0, tiled=True)


def to_all(block, axes):
    return exchange(jnp.broadcast_to(block, (lax.axis_size(axes), *block.shape)), axes)


def swap(array, axis):
    return lax.ppermute(array, axis, [(0, 1), (1, 0)])


def grade_rows(classes):
    levels = np.arange(classes, dtype=np.float32)
    rest = (np.float32(2.0) * levels / np.float32(classes - 1) - np.float32(1.0)) * np.sqrt(np.float32(3.0 / classes))
    rows = np.zeros((classes + 8, classes), np.float32)
    rows[:classes] = np.eye(classes)
    for k in range(3):
        rows[classes + k] = rest.astype(ml_dtypes.bfloat16).astype(np.float32)
        rest = rest - rows[classes + k]
    return rows.astype(ml_dtypes.bfloat16)


CROSS = (((1,), (1,)), ((), ()))


def score_kernel(last, scalars, own_docs_ref, near_docs_hbm, first_ref, second_ref, grades_ref, *refs):
    if last:
        before_ref, packed_ref, total, first, both, near_docs, arrived = refs
        own_docs = own_docs_ref
    else:
        total, first, both, near_docs, arrived = refs
        own_docs = own_docs_ref
    member = pl.program_id(0)
    which, parity = scalars[1], scalars[2]
    n_x, n_zc = first_ref.shape[0], first_ref.shape[1]
    _, depth = near_docs.shape
    width = first.shape[-1]
    classes = second_ref.shape[-1]
    fetch_near = pltpu.make_async_copy(near_docs_hbm, near_docs, arrived)

    @pl.when(member == 0)
    def _():
        fetch_near.start()

    at = 0 if last else member
    for x in range(n_x):
        for z in range(n_zc // 2):
            for core in range(2):
                first[z, x, core] = first_ref[x, 2 * z + core, at]
    rows = lax.dot_general(grades_ref[...], second_ref[0], CROSS, preferred_element_type=F32)
    direction = rows[classes : classes + 1] + rows[classes + 1 : classes + 2] + rows[classes + 2 : classes + 3]
    high = direction.astype(BF16).astype(F32)
    low = direction - high
    row = lax.broadcasted_iota(jnp.int32, (8, width), 0)
    slot = 2 * which + member
    along = jnp.where(row == slot, high, jnp.where(row == slot + 4, low, 0.0))
    both[...] = jnp.concatenate([rows[:classes], along], axis=0).astype(BF16)

    def add(k, docs):
        weight = first[...].reshape(depth, width)
        hidden = jnp.maximum(jnp.dot(docs, weight, preferred_element_type=F32), 0.0).astype(BF16)
        part = lax.dot_general(both[...], hidden, CROSS, preferred_element_type=F32)

        @pl.when(member == 0)
        def _():
            total[k] = part + before_ref[k] if last else part

        @pl.when(member > 0)
        def _():
            total[k] += part

    add(0, own_docs[...])

    @pl.when(member == 0)
    def _():
        fetch_near.wait()

    add(1, near_docs[...])
    if not last:
        return

    @pl.when(member == pl.num_programs(0) - 1)
    def _():
        n_y = packed_ref.shape[0] // 2
        quarter = classes // n_y
        for k in range(2):
            owner = (parity if k == 0 else 1 - parity) * n_y
            scores = total[k, classes : classes + 4] + total[k, classes + 4 : classes + 8]
            top = scores.astype(BF16).astype(F32)
            parts = jnp.concatenate([top, scores - top], axis=0).astype(BF16)
            for q in range(n_y):
                packed_ref[owner + q, :quarter] = total[k, quarter * q : quarter * (q + 1)].astype(BF16)
                packed_ref[owner + q, quarter:] = parts


def score(last, scalars, own_docs, near_docs, first, second, grades, n_y, *before):
    n_x, n_zc, members, rows, width = first.shape
    n_docs, depth = own_docs.shape
    classes = second.shape[-1]
    vmem = pl.BlockSpec(memory_space=pltpu.VMEM)
    hbm = pl.BlockSpec(memory_space=pltpu.HBM)
    totals = (2, classes + 8, n_docs)
    packed = (2 * n_y, classes // n_y + 8, n_docs)
    first_spec = pl.BlockSpec((n_x, n_zc, 1, rows, width), lambda m, s: (0, 0, m, 0, 0)) if last else vmem
    docs_scratch = [pltpu.VMEM((n_docs, depth), BF16), pltpu.SemaphoreType.DMA]
    scratch = [pltpu.VMEM((n_zc // 2, n_x, 2, rows, width), BF16), pltpu.VMEM((classes + 8, width), BF16)] + docs_scratch
    return pl.pallas_call(
        functools.partial(score_kernel, last),
        grid_spec=pltpu.PrefetchScalarGridSpec(
            num_scalar_prefetch=1,
            grid=(members,),
            in_specs=[
                vmem,
                hbm,
                first_spec,
                pl.BlockSpec((1, width, classes), lambda m, s: (s[0] + m, 0, 0)),
                vmem,
            ]
            + [vmem] * len(before),
            out_specs=vmem,
            scratch_shapes=[pltpu.VMEM(totals, F32)] * last + scratch,
        ),
        out_shape=jax.ShapeDtypeStruct(packed, BF16) if last else jax.ShapeDtypeStruct(totals, F32),
        compiler_params=pltpu.CompilerParams(dimension_semantics=("arbitrary",), vmem_limit_bytes=14 * 1024 * 1024),
    )(scalars, own_docs, near_docs, first, second, grades, *before)


def order_kernel(mine, *refs):
    *turn, out_ref = refs
    n_y = len(turn)
    quarters = []
    for q in range(n_y):
        back = lax.rem(mine[0] + n_y - q, n_y)
        quarter = turn[0][...].astype(F32)
        for k in range(1, n_y):
            quarter = jnp.where(back == k, turn[k][...].astype(F32), quarter)
        quarters.append(quarter)
    out_ref[...] = jnp.concatenate(quarters, axis=0).T


def in_order(mine, turn):
    rows, n_docs = turn[0].shape
    vmem = pl.BlockSpec(memory_space=pltpu.VMEM)
    return pl.pallas_call(
        order_kernel,
        in_specs=[pl.BlockSpec(memory_space=pltpu.SMEM)] + [vmem] * len(turn),
        out_specs=vmem,
        out_shape=jax.ShapeDtypeStruct((n_docs, rows * len(turn)), F32),
        compiler_params=pltpu.CompilerParams(vmem_limit_bytes=8 * 1024 * 1024),
    )(mine.reshape(1).astype(jnp.int32), *turn)


def halves(scores):
    high = lax.reduce_precision(scores, 8, 7)
    low = lax.reduce_precision(scores - high, 8, 7)
    return jnp.stack([high, low]).astype(BF16)


def step(embeddings, valid_mask, first_weight, second_weight, thresholds):
    members, rows, width = first_weight.shape
    n_docs = embeddings.shape[0]
    z_axes = ("za", "zp")
    n_za, n_y = lax.axis_size("za"), lax.axis_size("y")
    parity, core = lax.axis_index("zp"), lax.axis_index("core")
    half, pair = members // 2, members // 4

    blocks = first_weight.reshape(1, 4, pair, rows, width)
    blocks = jnp.broadcast_to(blocks, (n_za, *blocks.shape[1:])).reshape(n_za * 4, pair, rows, width)
    along_z = exchange(blocks, ("za", "zp", "core"))
    docs = embeddings
    docs_near = swap(docs, "zp")
    first_a = to_all(along_z, "x")
    first_b = swap(first_a, "core")
    classes = second_weight.shape[2]
    grades = jnp.asarray(grade_rows(classes))

    def scored(last, first, which, *before):
        scalars = jnp.stack([parity * half + which * pair, which, parity]).astype(jnp.int32)
        return score(last, scalars, docs, docs_near, first, second_weight, grades, n_y, *before)

    total_a = scored(False, first_a, core)
    packed = scored(True, first_b, 1 - core, total_a)

    quarter = classes // n_y
    blocks = exchange(packed, ("zp", "y"))
    part_mean = lax.reduce_precision(jnp.sum(blocks[:, :quarter].astype(F32), axis=0), 8, 7).astype(BF16)
    part_scores = blocks[:, quarter:].astype(F32).reshape(2, n_y, 2, half, n_docs).sum(axis=(1, 2)).reshape(members, n_docs)
    message = jnp.concatenate([part_mean, halves(part_scores).reshape(2 * members, n_docs)], axis=0)
    answer = swap(message, "zh")
    total = message.astype(F32) + answer.astype(F32)
    mean_quarter = (total[:quarter] * (1.0 / members)).astype(BF16)
    turn = [mean_quarter]
    for k in range(1, n_y):
        turn.append(lax.ppermute(mean_quarter, "y", [(i, (i + k) % n_y) for i in range(n_y)]))
    mean_logits = in_order(lax.axis_index("y"), turn)
    scores = total[quarter : quarter + members] + total[quarter + members :]

    cutoffs = thresholds.astype(F32) / 256.0
    validity = valid_mask.astype(F32)
    kept_soft = validity[None, :] * jax.nn.sigmoid(4.0 * (scores - cutoffs[:, None]))
    ens_score = jnp.sum(scores, axis=0) / members
    ens_kept = jax.nn.sigmoid(4.0 * (ens_score - jnp.mean(cutoffs)))
    counts = jnp.stack([jnp.sum(kept_soft, axis=1), jnp.sum(kept_soft * ens_kept[None, :], axis=1)])
    counts = to_all(counts, ("x", "core")).sum(axis=0)
    counts = to_all(counts, z_axes).sum(axis=0)
    member = lax.axis_index("y") * 2 + lax.axis_index("zh")
    shares = lax.dynamic_slice_in_dim(counts, member, 1, 1) / n_docs
    return mean_logits, shares[0], shares[1]


def solution(mesh):
    devices = mesh.devices.reshape(4, 2, 4, 2, 4, 2)
    fine = Mesh(devices, ("za", "zp", "x", "core", "y", "zh"))
    dp, ens = ("za", "zp", "x", "core"), ("y", "zh")
    return jax.shard_map(
        step,
        mesh=fine,
        in_specs=(P(dp, None), P(dp), P(None, dp, ens), P(None, ens, None), P()),
        out_specs=(P(dp, None), P(ens), P(ens)),
        check_vma=False,
    )
```

```python
import functools

import jax
import jax.numpy as jnp
import ml_dtypes
import numpy as np
from jax import lax
from jax.experimental import pallas as pl
from jax.experimental.pallas import tpu as pltpu
from jax.sharding import Mesh, PartitionSpec as P


F32 = jnp.float32
BF16 = jnp.bfloat16


def exchange(blocks, axes):
    return lax.all_to_all(blocks, axes, split_axis=0, concat_axis=0, tiled=True)


def to_all(block, axes):
    return exchange(jnp.broadcast_to(block, (lax.axis_size(axes), *block.shape)), axes)


def swap(array, axis):
    return lax.ppermute(array, axis, [(0, 1), (1, 0)])


def grade_rows(classes):
    levels = np.arange(classes, dtype=np.float32)
    rest = (np.float32(2.0) * levels / np.float32(classes - 1) - np.float32(1.0)) * np.sqrt(np.float32(3.0 / classes))
    rows = np.zeros((classes + 8, classes), np.float32)
    rows[:classes] = np.eye(classes)
    for k in range(3):
        rows[classes + k] = rest.astype(ml_dtypes.bfloat16).astype(np.float32)
        rest = rest - rows[classes + k]
    return rows.astype(ml_dtypes.bfloat16)


CROSS = (((1,), (1,)), ((), ()))


def score_kernel(last, scalars, own_docs_ref, near_docs_hbm, first_ref, second_ref, grades_ref, *refs):
    if last:
        before_ref, packed_ref, total, first, both, near_docs, arrived = refs
        own_docs = own_docs_ref
    else:
        total, first, both, near_docs, arrived = refs
        own_docs = own_docs_ref
    member = pl.program_id(0)
    which, parity = scalars[1], scalars[2]
    n_x, n_zc = first_ref.shape[0], first_ref.shape[1]
    _, depth = near_docs.shape
    width = first.shape[-1]
    classes = second_ref.shape[-1]
    fetch_near = pltpu.make_async_copy(near_docs_hbm, near_docs, arrived)

    @pl.when(member == 0)
    def _():
        fetch_near.start()

    at = 0 if last else member
    for x in range(n_x):
        for z in range(n_zc // 2):
            for core in range(2):
                first[z, x, core] = first_ref[x, 2 * z + core, at]
    rows = lax.dot_general(grades_ref[...], second_ref[0], CROSS, preferred_element_type=F32)
    direction = rows[classes : classes + 1] + rows[classes + 1 : classes + 2] + rows[classes + 2 : classes + 3]
    high = direction.astype(BF16).astype(F32)
    low = direction - high
    row = lax.broadcasted_iota(jnp.int32, (8, width), 0)
    slot = 2 * which + member
    along = jnp.where(row == slot, high, jnp.where(row == slot + 4, low, 0.0))
    both[...] = jnp.concatenate([rows[:classes], along], axis=0).astype(BF16)

    def add(k, docs):
        weight = first[...].reshape(depth, width)
        hidden = jnp.maximum(jnp.dot(docs, weight, preferred_element_type=F32), 0.0).astype(BF16)
        part = lax.dot_general(both[...], hidden, CROSS, preferred_element_type=F32)

        @pl.when(member == 0)
        def _():
            total[k] = part + before_ref[k] if last else part

        @pl.when(member > 0)
        def _():
            total[k] += part

    add(0, own_docs[...])

    @pl.when(member == 0)
    def _():
        fetch_near.wait()

    add(1, near_docs[...])
    if not last:
        return

    @pl.when(member == pl.num_programs(0) - 1)
    def _():
        n_y = packed_ref.shape[0] // 2
        quarter = classes // n_y
        for k in range(2):
            owner = (parity if k == 0 else 1 - parity) * n_y
            scores = total[k, classes : classes + 4] + total[k, classes + 4 : classes + 8]
            top = scores.astype(BF16).astype(F32)
            parts = jnp.concatenate([top, scores - top], axis=0).astype(BF16)
            for q in range(n_y):
                packed_ref[owner + q, :quarter] = total[k, quarter * q : quarter * (q + 1)].astype(BF16)
                packed_ref[owner + q, quarter:] = parts


def score(last, scalars, own_docs, near_docs, first, second, grades, n_y, *before):
    n_x, n_zc, members, rows, width = first.shape
    n_docs, depth = own_docs.shape
    classes = second.shape[-1]
    vmem = pl.BlockSpec(memory_space=pltpu.VMEM)
    hbm = pl.BlockSpec(memory_space=pltpu.HBM)
    totals = (2, classes + 8, n_docs)
    packed = (2 * n_y, classes // n_y + 8, n_docs)
    first_spec = pl.BlockSpec((n_x, n_zc, 1, rows, width), lambda m, s: (0, 0, m, 0, 0)) if last else vmem
    docs_scratch = [pltpu.VMEM((n_docs, depth), BF16), pltpu.SemaphoreType.DMA]
    scratch = [pltpu.VMEM((n_zc // 2, n_x, 2, rows, width), BF16), pltpu.VMEM((classes + 8, width), BF16)] + docs_scratch
    return pl.pallas_call(
        functools.partial(score_kernel, last),
        grid_spec=pltpu.PrefetchScalarGridSpec(
            num_scalar_prefetch=1,
            grid=(members,),
            in_specs=[
                vmem,
                hbm,
                first_spec,
                pl.BlockSpec((1, width, classes), lambda m, s: (s[0] + m, 0, 0)),
                vmem,
            ]
            + [vmem] * len(before),
            out_specs=vmem,
            scratch_shapes=[pltpu.VMEM(totals, F32)] * last + scratch,
        ),
        out_shape=jax.ShapeDtypeStruct(packed, BF16) if last else jax.ShapeDtypeStruct(totals, F32),
        compiler_params=pltpu.CompilerParams(dimension_semantics=("arbitrary",), vmem_limit_bytes=14 * 1024 * 1024),
    )(scalars, own_docs, near_docs, first, second, grades, *before)


def stage_kernel(docs_hbm, out_ref, arrived):
    fetch = pltpu.make_async_copy(docs_hbm, out_ref, arrived)
    fetch.start()
    fetch.wait()


def staged(docs):
    return pl.pallas_call(
        stage_kernel,
        in_specs=[pl.BlockSpec(memory_space=pltpu.HBM)],
        out_specs=pl.BlockSpec(memory_space=pltpu.VMEM),
        scratch_shapes=[pltpu.SemaphoreType.DMA],
        out_shape=jax.ShapeDtypeStruct(docs.shape, docs.dtype),
        compiler_params=pltpu.CompilerParams(vmem_limit_bytes=4 * 1024 * 1024),
    )(docs)


def order_kernel(mine, near_ref, far_ref, out_ref):
    odd = mine[0] % 2
    high = mine[0] // 2
    rows = near_ref.shape[0] // 2
    near = [near_ref[:rows].astype(F32), near_ref[rows:].astype(F32)]
    far = [far_ref[:rows].astype(F32), far_ref[rows:].astype(F32)]
    near = [jnp.where(odd == k, near[0], near[1]) for k in range(2)]
    far = [jnp.where(odd == k, far[1], far[0]) for k in range(2)]
    low = [jnp.where(high == 0, near[k], far[k]) for k in range(2)]
    top = [jnp.where(high == 0, far[k], near[k]) for k in range(2)]
    out_ref[...] = jnp.concatenate(low + top, axis=0).T


def in_order(mine, near, far):
    rows, n_docs = near.shape
    vmem = pl.BlockSpec(memory_space=pltpu.VMEM)
    return pl.pallas_call(
        order_kernel,
        in_specs=[pl.BlockSpec(memory_space=pltpu.SMEM), vmem, vmem],
        out_specs=vmem,
        out_shape=jax.ShapeDtypeStruct((n_docs, 2 * rows), F32),
        compiler_params=pltpu.CompilerParams(vmem_limit_bytes=8 * 1024 * 1024),
    )(mine.reshape(1).astype(jnp.int32), near, far)


def halves(scores):
    high = lax.reduce_precision(scores, 8, 7)
    low = lax.reduce_precision(scores - high, 8, 7)
    return jnp.stack([high, low]).astype(BF16)


def step(embeddings, valid_mask, first_weight, second_weight, thresholds):
    members, rows, width = first_weight.shape
    n_docs = embeddings.shape[0]
    z_axes = ("za", "zp")
    n_za, n_y = lax.axis_size("za"), lax.axis_size("y")
    parity, core = lax.axis_index("zp"), lax.axis_index("core")
    half, pair = members // 2, members // 4

    blocks = first_weight.reshape(1, 4, pair, rows, width)
    blocks = jnp.broadcast_to(blocks, (n_za, *blocks.shape[1:])).reshape(n_za * 4, pair, rows, width)
    along_z = exchange(blocks, ("za", "zp", "core"))
    docs = staged(embeddings)
    docs_near = swap(embeddings, "zp")
    first_a = to_all(along_z, "x")
    first_b = swap(first_a, "core")
    classes = second_weight.shape[2]
    grades = jnp.asarray(grade_rows(classes))

    def scored(last, first, which, *before):
        scalars = jnp.stack([parity * half + which * pair, which, parity]).astype(jnp.int32)
        return score(last, scalars, docs, docs_near, first, second_weight, grades, n_y, *before)

    total_a = scored(False, first_a, core)
    packed = scored(True, first_b, 1 - core, total_a)

    quarter = classes // n_y
    blocks = exchange(packed, ("zp", "y"))
    part_mean = lax.reduce_precision(jnp.sum(blocks[:, :quarter].astype(F32), axis=0), 8, 7).astype(BF16)
    part_scores = blocks[:, quarter:].astype(F32).reshape(2, n_y, 2, half, n_docs).sum(axis=(1, 2)).reshape(members, n_docs)
    message = jnp.concatenate([part_mean, halves(part_scores).reshape(2 * members, n_docs)], axis=0)
    answer = swap(message, "zh")
    total = message.astype(F32) + answer.astype(F32)
    mean_quarter = (total[:quarter] * (1.0 / members)).astype(BF16)
    paired = lax.ppermute(mean_quarter, "y", [(i, i ^ 1) for i in range(n_y)])
    pair_rows = jnp.concatenate([mean_quarter, paired], axis=0)
    crossed = lax.ppermute(pair_rows, "y", [(i, n_y - 1 - i) for i in range(n_y)])
    mean_logits = in_order(lax.axis_index("y"), pair_rows, crossed)
    scores = total[quarter : quarter + members] + total[quarter + members :]

    cutoffs = thresholds.astype(F32) / 256.0
    validity = valid_mask.astype(F32)
    kept_soft = validity[None, :] * jax.nn.sigmoid(4.0 * (scores - cutoffs[:, None]))
    ens_score = jnp.sum(scores, axis=0) / members
    ens_kept = jax.nn.sigmoid(4.0 * (ens_score - jnp.mean(cutoffs)))
    counts = jnp.stack([jnp.sum(kept_soft, axis=1), jnp.sum(kept_soft * ens_kept[None, :], axis=1)])
    counts = to_all(counts, ("x", "core")).sum(axis=0)
    counts = to_all(counts, z_axes).sum(axis=0)
    member = lax.axis_index("y") * 2 + lax.axis_index("zh")
    shares = lax.dynamic_slice_in_dim(counts, member, 1, 1) / n_docs
    return mean_logits, shares[0], shares[1]


def solution(mesh):
    devices = mesh.devices.reshape(4, 2, 4, 2, 4, 2)
    fine = Mesh(devices, ("za", "zp", "x", "core", "y", "zh"))
    dp, ens = ("za", "zp", "x", "core"), ("y", "zh")
    return jax.shard_map(
        step,
        mesh=fine,
        in_specs=(P(dp, None), P(dp), P(None, dp, ens), P(None, ens, None), P()),
        out_specs=(P(dp, None), P(ens), P(ens)),
        check_vma=False,
    )
```

```python
import functools

import jax
import jax.numpy as jnp
import ml_dtypes
import numpy as np
from jax import lax
from jax.experimental import pallas as pl
from jax.experimental.pallas import tpu as pltpu
from jax.sharding import Mesh, PartitionSpec as P


F32 = jnp.float32
BF16 = jnp.bfloat16


def exchange(blocks, axes):
    return lax.all_to_all(blocks, axes, split_axis=0, concat_axis=0, tiled=True)


def to_all(block, axes):
    return exchange(jnp.broadcast_to(block, (lax.axis_size(axes), *block.shape)), axes)


def swap(array, axis):
    return lax.ppermute(array, axis, [(0, 1), (1, 0)])


def grade_rows(classes):
    levels = np.arange(classes, dtype=np.float32)
    rest = (np.float32(2.0) * levels / np.float32(classes - 1) - np.float32(1.0)) * np.sqrt(np.float32(3.0 / classes))
    rows = np.zeros((classes + 8, classes), np.float32)
    rows[:classes] = np.eye(classes)
    for k in range(3):
        rows[classes + k] = rest.astype(ml_dtypes.bfloat16).astype(np.float32)
        rest = rest - rows[classes + k]
    return rows.astype(ml_dtypes.bfloat16)


CROSS = (((1,), (1,)), ((), ()))


def score_kernel(last, scalars, own_docs_ref, near_docs_hbm, first_ref, second_ref, grades_ref, *refs):
    if last:
        before_ref, packed_ref, total, first, both, near_docs, arrived = refs
        own_docs = own_docs_ref
    else:
        total, first, both, near_docs, arrived = refs
        own_docs = own_docs_ref
    member = pl.program_id(0)
    which, parity = scalars[1], scalars[2]
    n_x, n_zc = first_ref.shape[0], first_ref.shape[1]
    _, depth = near_docs.shape
    width = first.shape[-1]
    classes = second_ref.shape[-1]
    fetch_near = pltpu.make_async_copy(near_docs_hbm, near_docs, arrived)

    @pl.when(member == 0)
    def _():
        fetch_near.start()

    at = 0 if last else member
    for x in range(n_x):
        for z in range(n_zc // 2):
            for core in range(2):
                first[z, x, core] = first_ref[x, 2 * z + core, at]
    rows = lax.dot_general(grades_ref[...], second_ref[0], CROSS, preferred_element_type=F32)
    direction = rows[classes : classes + 1] + rows[classes + 1 : classes + 2] + rows[classes + 2 : classes + 3]
    high = direction.astype(BF16).astype(F32)
    low = direction - high
    row = lax.broadcasted_iota(jnp.int32, (8, width), 0)
    slot = 2 * which + member
    along = jnp.where(row == slot, high, jnp.where(row == slot + 4, low, 0.0))
    both[...] = jnp.concatenate([rows[:classes], along], axis=0).astype(BF16)

    def add(k, docs):
        weight = first[...].reshape(depth, width)
        hidden = jnp.maximum(jnp.dot(docs, weight, preferred_element_type=F32), 0.0).astype(BF16)
        part = lax.dot_general(both[...], hidden, CROSS, preferred_element_type=F32)

        @pl.when(member == 0)
        def _():
            total[k] = part + before_ref[k] if last else part

        @pl.when(member > 0)
        def _():
            total[k] += part

    add(0, own_docs[...])

    @pl.when(member == 0)
    def _():
        fetch_near.wait()

    add(1, near_docs[...])
    if not last:
        return

    @pl.when(member == pl.num_programs(0) - 1)
    def _():
        n_y = packed_ref.shape[0] // 2
        quarter = classes // n_y
        for k in range(2):
            owner = (parity if k == 0 else 1 - parity) * n_y
            scores = total[k, classes : classes + 4] + total[k, classes + 4 : classes + 8]
            top = scores.astype(BF16).astype(F32)
            parts = jnp.concatenate([top, scores - top], axis=0).astype(BF16)
            for q in range(n_y):
                packed_ref[owner + q, :quarter] = total[k, quarter * q : quarter * (q + 1)].astype(BF16)
                packed_ref[owner + q, quarter:] = parts


def score(last, scalars, own_docs, near_docs, first, second, grades, n_y, *before):
    n_x, n_zc, members, rows, width = first.shape
    n_docs, depth = own_docs.shape
    classes = second.shape[-1]
    vmem = pl.BlockSpec(memory_space=pltpu.VMEM)
    hbm = pl.BlockSpec(memory_space=pltpu.HBM)
    totals = (2, classes + 8, n_docs)
    packed = (2 * n_y, classes // n_y + 8, n_docs)
    first_spec = pl.BlockSpec((n_x, n_zc, 1, rows, width), lambda m, s: (0, 0, m, 0, 0)) if last else vmem
    docs_scratch = [pltpu.VMEM((n_docs, depth), BF16), pltpu.SemaphoreType.DMA]
    scratch = [pltpu.VMEM((n_zc // 2, n_x, 2, rows, width), BF16), pltpu.VMEM((classes + 8, width), BF16)] + docs_scratch
    return pl.pallas_call(
        functools.partial(score_kernel, last),
        grid_spec=pltpu.PrefetchScalarGridSpec(
            num_scalar_prefetch=1,
            grid=(members,),
            in_specs=[
                vmem,
                hbm,
                first_spec,
                pl.BlockSpec((1, width, classes), lambda m, s: (s[0] + m, 0, 0)),
                vmem,
            ]
            + [vmem] * len(before),
            out_specs=vmem,
            scratch_shapes=[pltpu.VMEM(totals, F32)] * last + scratch,
        ),
        out_shape=jax.ShapeDtypeStruct(packed, BF16) if last else jax.ShapeDtypeStruct(totals, F32),
        compiler_params=pltpu.CompilerParams(dimension_semantics=("arbitrary",), vmem_limit_bytes=22 * 1024 * 1024),
    )(scalars, own_docs, near_docs, first, second, grades, *before)


def stage_kernel(docs_hbm, out_ref, arrived):
    fetch = pltpu.make_async_copy(docs_hbm, out_ref, arrived)
    fetch.start()
    fetch.wait()


def staged(docs):
    return pl.pallas_call(
        stage_kernel,
        in_specs=[pl.BlockSpec(memory_space=pltpu.HBM)],
        out_specs=pl.BlockSpec(memory_space=pltpu.VMEM),
        scratch_shapes=[pltpu.SemaphoreType.DMA],
        out_shape=jax.ShapeDtypeStruct(docs.shape, docs.dtype),
        compiler_params=pltpu.CompilerParams(vmem_limit_bytes=4 * 1024 * 1024),
    )(docs)


def order_kernel(mine, near_ref, far_ref, out_ref):
    odd = mine[0] % 2
    high = mine[0] // 2
    rows = near_ref.shape[0] // 2
    near = [near_ref[:rows].astype(F32), near_ref[rows:].astype(F32)]
    far = [far_ref[:rows].astype(F32), far_ref[rows:].astype(F32)]
    near = [jnp.where(odd == k, near[0], near[1]) for k in range(2)]
    far = [jnp.where(odd == k, far[1], far[0]) for k in range(2)]
    low = [jnp.where(high == 0, near[k], far[k]) for k in range(2)]
    top = [jnp.where(high == 0, far[k], near[k]) for k in range(2)]
    out_ref[...] = jnp.concatenate(low + top, axis=0).T


def in_order(mine, near, far):
    rows, n_docs = near.shape
    vmem = pl.BlockSpec(memory_space=pltpu.VMEM)
    return pl.pallas_call(
        order_kernel,
        in_specs=[pl.BlockSpec(memory_space=pltpu.SMEM), vmem, vmem],
        out_specs=vmem,
        out_shape=jax.ShapeDtypeStruct((n_docs, 2 * rows), F32),
        compiler_params=pltpu.CompilerParams(vmem_limit_bytes=8 * 1024 * 1024),
    )(mine.reshape(1).astype(jnp.int32), near, far)


def halves(scores):
    high = lax.reduce_precision(scores, 8, 7)
    low = lax.reduce_precision(scores - high, 8, 7)
    return jnp.stack([high, low]).astype(BF16)


def step(embeddings, valid_mask, first_weight, second_weight, thresholds):
    members, rows, width = first_weight.shape
    n_docs = embeddings.shape[0]
    n_za, n_y = lax.axis_size("za"), lax.axis_size("y")
    parity, core = lax.axis_index("zp"), lax.axis_index("core")
    half, pair = members // 2, members // 4

    blocks = first_weight.reshape(1, 4, pair, rows, width)
    blocks = jnp.broadcast_to(blocks, (n_za, *blocks.shape[1:])).reshape(n_za * 4, pair, rows, width)
    along_z = exchange(blocks, ("za", "zp", "core"))
    docs = staged(embeddings)
    docs_near = swap(embeddings, "zp")
    first_a = to_all(along_z, "x")
    first_b = swap(first_a, "core")
    classes = second_weight.shape[2]
    grades = jnp.asarray(grade_rows(classes))

    def scored(last, first, which, *before):
        scalars = jnp.stack([parity * half + which * pair, which, parity]).astype(jnp.int32)
        return score(last, scalars, docs, docs_near, first, second_weight, grades, n_y, *before)

    total_a = scored(False, first_a, core)
    packed = scored(True, first_b, 1 - core, total_a)

    quarter = classes // n_y
    blocks = exchange(packed, ("zp", "y"))
    part_mean = lax.reduce_precision(jnp.sum(blocks[:, :quarter].astype(F32), axis=0), 8, 7).astype(BF16)
    part_scores = blocks[:, quarter:].astype(F32).reshape(2, n_y, 2, half, n_docs).sum(axis=(1, 2)).reshape(members, n_docs)
    message = jnp.concatenate([part_mean, halves(part_scores).reshape(2 * members, n_docs)], axis=0)
    answer = swap(message, "zh")
    total = message.astype(F32) + answer.astype(F32)
    mean_quarter = (total[:quarter] * (1.0 / members)).astype(BF16)
    paired = lax.ppermute(mean_quarter, "y", [(i, i ^ 1) for i in range(n_y)])
    pair_rows = jnp.concatenate([mean_quarter, paired], axis=0)
    crossed = lax.ppermute(pair_rows, "y", [(i, n_y - 1 - i) for i in range(n_y)])
    mean_logits = in_order(lax.axis_index("y"), pair_rows, crossed)
    scores = total[quarter : quarter + members] + total[quarter + members :]

    cutoffs = thresholds.astype(F32) / 256.0
    validity = valid_mask.astype(F32)
    kept_soft = validity[None, :] * jax.nn.sigmoid(4.0 * (scores - cutoffs[:, None]))
    ens_score = jnp.sum(scores, axis=0) / members
    ens_kept = jax.nn.sigmoid(4.0 * (ens_score - jnp.mean(cutoffs)))
    counts = jnp.stack([jnp.sum(kept_soft, axis=1), jnp.sum(kept_soft * ens_kept[None, :], axis=1)])
    counts = to_all(counts, ("zp", "x", "core")).sum(axis=0)
    counts = to_all(counts, "za").sum(axis=0)
    member = lax.axis_index("y") * 2 + lax.axis_index("zh")
    shares = lax.dynamic_slice_in_dim(counts, member, 1, 1) / n_docs
    return mean_logits, shares[0], shares[1]


def solution(mesh):
    devices = mesh.devices.reshape(4, 2, 4, 2, 4, 2)
    fine = Mesh(devices, ("za", "zp", "x", "core", "y", "zh"))
    dp, ens = ("za", "zp", "x", "core"), ("y", "zh")
    return jax.shard_map(
        step,
        mesh=fine,
        in_specs=(P(dp, None), P(dp), P(None, dp, ens), P(None, ens, None), P()),
        out_specs=(P(dp, None), P(ens), P(ens)),
        check_vma=False,
    )
```
